32 devices in a mesh: freq: 4 (over x, core), gblk: 8 (over z, y).
Axes of the slice: x: 2, y: 2, z: 4, core: 2. Of those that a mesh axis runs over, the one named last changes fastest.
Arguments:
- w_imag: bfloat16 [8, 8192, 16384], P('freq', 'gblk'), may hold values from -0.046875 to 0.046875
- w_real: bfloat16 [4, 8192, 16384], P('freq', 'gblk'), may hold values from -0.046875 to 0.046875
- pair_elements: bfloat16 [8192, 256], P('gblk'), may hold values from -0.75 to 0.75
- quad_weight: float32 [8, 128], P('freq'), may hold values from 0.1 to 1
- residue_freq: int32 [128], replicated, may hold values from 0 to 3
- owner_bands: int32 [128], replicated, may hold values from 0 to 127, each once
Outputs:
- sigma: float32 [128, 256], P(('freq', 'gblk'))
The draws below stay inside these ranges and needn't reach their ends.
Inputs may be any that keep to these rules, and one draw needn't show every extreme that they name: `owner_bands`: each band appears once.
All inputs are finite; a program needn't handle non-finite values.
Results may differ from the reference program's by a relative error of at most 0.0003.
Values may be sent and summed in bfloat16 or wider, within the bound.
A program may use at most 192 MiB of HBM per device.

```python
import math
import jax
import jax.numpy as jnp
from jax import lax

NG = 8192
NB = 128
NFI = 8
NFR = 4


def set_ends(result, stream_key, low, top_value):
    longest = result.shape.index(max(result.shape))
    spots = []
    for shift in (0, 1):
        where = [jax.random.randint(jax.random.fold_in(stream_key, axis), (), 0, length) for axis, length in enumerate(result.shape)]
        where[longest] = (where[longest] + shift) % result.shape[longest]
        spots.append(tuple(where))
    return result.at[spots[0]].set(low).at[spots[1]].set(top_value)


def strengthened(values, stream_key, source, target, blocks, factor):
    owner, partner = [(jnp.arange(values.shape[position]) // (values.shape[position] // blocks)).reshape([-1 if axis == position else 1 for axis in range(values.ndim)]) for position in (source, target)]
    chosen = jax.random.permutation(stream_key, blocks)[partner]
    strong = (owner == chosen) | (owner == (partner + blocks // 2) % blocks)
    return jnp.where(strong, factor * values, values)


def block_scale(stream_key, extent, shards, smallest, largest):
    def one(dim, parts):
        steps = jax.random.uniform(jax.random.fold_in(jax.random.fold_in(stream_key, 6), dim), (parts,), jnp.float32, smallest / len(shards), largest / len(shards))
        return jnp.repeat(jnp.exp(steps), extent[dim] // parts).reshape((-1,) + (1,) * (len(extent) - dim - 1))

    factor_of = one(*shards[0])
    for cut in shards[1:]:
        factor_of = factor_of * one(*cut)
    return factor_of


def scatter_about(rng, dims, spread, reach, split=(), held_as=jnp.bfloat16):
    loudness = block_scale(rng, dims, split, -0.22, 0.18) if split else 1.0
    entries = jax.random.normal(rng, dims, jnp.float32) * spread * loudness
    return jnp.minimum(jnp.maximum(entries, -reach), reach).astype(held_as)


def noise_with(rng, dims, scale, limit, cuts, heavy, kind=jnp.bfloat16):
    drawn = scale * jax.random.normal(rng, dims, jnp.float32)
    if cuts:
        drawn = drawn * block_scale(rng, dims, cuts, -0.22, 0.18)
    return jnp.clip(strengthened(drawn, jax.random.fold_in(rng, 3), *heavy), -limit, limit).astype(kind)


def setup_inputs(seed: int = 0) -> dict:
    keys = jax.random.split(jax.random.key(seed), 7)
    w_imag = scatter_about(keys[0], (NFI, NG, 2 * NG), (2 * NG) ** -0.5, 0.046875, ((0, 4), (1, 8)))
    w_real = scatter_about(keys[1], (NFR, NG, 2 * NG), (2 * NG) ** -0.5, 0.046875, ((0, 4), (1, 8)))
    pair_elements = noise_with(keys[2], (NG, 2 * NB), 0.09, 0.75, ((0, 8),), (0, 1, 8, 2.0))
    quad_weight = jnp.clip(jnp.exp(math.log(1.0) - 2.3025851 * jax.random.uniform(keys[3], (NFI, NB), jnp.float32) ** block_scale(keys[3], (NFI, NB), ((0, 4),), -0.2, 0.2)), 0.1, 1.0)
    residue_freq = set_ends(jax.random.randint(keys[4], (NB,), 0, NFR), jax.random.fold_in(keys[4], 1), 0, NFR - 1).astype(jnp.int32)
    owner_bands = jax.random.permutation(keys[5], NB).astype(jnp.int32)
    return {"w_imag": w_imag, "w_real": w_real, "pair_elements": pair_elements, "quad_weight": quad_weight, "residue_freq": residue_freq, "owner_bands": owner_bands}


def reference(w_imag, w_real, pair_elements, quad_weight, residue_freq, owner_bands):
    bands = NB
    real_part = pair_elements[:, :bands]
    imag_part = pair_elements[:, bands:]
    lower_rows = jnp.concatenate([-imag_part, real_part], axis=1)
    stacked = jnp.concatenate([pair_elements, lower_rows], axis=0).astype(jnp.float32)
    block_rows = min(NG, 1024)
    wide_elems = pair_elements.astype(jnp.float32).reshape(NG // block_rows, block_rows, 2 * bands)

    def per_frequency(matrix):
        pieces = matrix.reshape(NG // block_rows, block_rows, 2 * NG)

        def per_block(packed):
            w_block, m_block = packed
            x_block = jnp.dot(w_block.astype(jnp.float32), stacked, precision=lax.Precision.HIGHEST)
            return jnp.dot(m_block.T, x_block, precision=lax.Precision.HIGHEST)

        blocks = jnp.sum(lax.map(per_block, (pieces, wide_elems)), axis=0)
        sig_re = blocks[:bands, :bands] + blocks[bands:, bands:]
        sig_im = blocks[:bands, bands:] - blocks[bands:, :bands]
        return jnp.concatenate([sig_re, sig_im], axis=1)

    s_imag = lax.map(per_frequency, w_imag)
    s_real = lax.map(per_frequency, w_real)
    residue_weight = (residue_freq[None, :] == jnp.arange(NFR, dtype=jnp.int32)[:, None]).astype(jnp.float32)
    total = jnp.sum(quad_weight[:, :, None] * s_imag, axis=0) + jnp.sum(residue_weight[:, :, None] * s_real, axis=0)
    return total[owner_bands]
```

```python
import functools
import math

import jax
import jax.numpy as jnp
from jax import lax
from jax.experimental import pallas as pl
from jax.experimental.pallas import tpu as pltpu
from jax.sharding import PartitionSpec as P

MESH = pl.DeviceIdType.MESH
LANES = 256
BUFFERS = 3


def ring_position(index, n):
    z = index // 2
    return z + (index % 2) * (n - 1 - 2 * z)


def ring_index(position, n):
    low = (position < n // 2).astype(jnp.int32)
    return low * (2 * position) + (1 - low) * (2 * (n - 1 - position) + 1)


def self_energy_kernel(
    n, nf, pieces_half, tile,
    wi_hbm, wr_hbm, m_hbm, quad_ref, residue_ref, owner_ref, out_ref,
    wbuf, gath, left, weights, ubuf, acc, stage, inbox,
    w_sem, own_sem, ring_send, ring_recv, pair_send, pair_recv, out_send, out_recv,
):
    f = lax.axis_index("freq")
    me = lax.axis_index("gblk")
    pos = ring_position(me, n)
    core = f % 2
    fi, rows, width = wi_hbm.shape
    fr = wr_hbm.shape[0]
    g_count = width // 2
    bands = owner_ref.shape[1]
    piece_rows = gath.shape[2]
    per_block = rows // tile
    steps = n * per_block
    lag = min(2 * per_block, steps - 1)
    devices = n * nf
    mine = f * n + me

    def slot_of(k):
        d = (k + 1) // 2
        sign = 2 * (k % 2) - 1
        return lax.rem(pos - sign * d + 2 * n, n)

    def w_copies(t, slot):
        block = ring_index(slot_of(t // per_block), n)
        col = block * rows + (t % per_block) * tile
        copies = []
        for half in range(2):
            cols = pl.ds(pl.multiple_of(col + half * g_count, tile), tile)
            copies.append(pltpu.make_async_copy(
                wi_hbm.at[:, :, cols], wbuf.at[slot, half, pl.ds(0, fi)], w_sem.at[slot, half, 0]))
            copies.append(pltpu.make_async_copy(
                wr_hbm.at[:, :, cols], wbuf.at[slot, half, pl.ds(fi, fr)], w_sem.at[slot, half, 1]))
        return copies

    barrier = pltpu.get_barrier_semaphore()

    def greet(r, carry):
        other = lax.rem(mine + r, devices)
        pl.semaphore_signal(barrier, inc=1, device_id=(other // n, other % n), device_id_type=MESH)
        return carry

    lax.fori_loop(1, devices, greet, 0)

    own = [pltpu.make_async_copy(
        m_hbm.at[pl.ds(i * piece_rows, piece_rows)], gath.at[pos, i], own_sem.at[i])
        for i in range(2 * pieces_half)]
    for c in own:
        c.start()
    for t in range(min(BUFFERS - 1, steps)):
        for c in w_copies(t, t):
            c.start()

    onehot_t = (lax.broadcasted_iota(jnp.int32, (bands, bands), 0) == owner_ref[...]).astype(jnp.float32)
    onehot = jnp.transpose(onehot_t)
    first = f * fr
    for j in range(fi):
        weights[j] = jnp.sum(onehot * quad_ref[pl.ds(j, 1), :], axis=1, keepdims=True)
    for j in range(fr):
        row = (residue_ref[...] == first + j).astype(jnp.float32)
        weights[fi + j] = jnp.sum(onehot * row, axis=1, keepdims=True)
    acc[...] = jnp.zeros_like(acc)
    for c in own:
        c.wait()
    own_m = gath[pos].reshape(rows, 2 * bands)
    picker = onehot.astype(jnp.bfloat16)
    for half in range(2):
        left[pl.ds(half * bands, bands), :] = lax.dot_general(
            picker, own_m[:, half * bands:(half + 1) * bands], (((1,), (1,)), ((), ())),
            preferred_element_type=jnp.float32).astype(jnp.bfloat16)

    split = (pieces_half + 1) // 2

    def direction(k, q):
        if k == n - 1:
            return 1 if q < split or n == 2 else -1
        return 1 if k % 2 else -1

    def ring_copy(k, q, sending_slot, sign):
        to = ring_index(lax.rem(pos + sign + n, n), n)
        at = gath.at[sending_slot, core * pieces_half + q]
        return pltpu.make_async_remote_copy(
            src_ref=at, dst_ref=at, send_sem=ring_send.at[k, q], recv_sem=ring_recv.at[k, q],
            device_id=(f, to), device_id_type=MESH)

    def pair_copy(k, q, whose):
        at = gath.at[slot_of(k), whose * pieces_half + q]
        return pltpu.make_async_remote_copy(
            src_ref=at, dst_ref=at, send_sem=pair_send.at[k, q], recv_sem=pair_recv.at[k, q],
            device_id=(f + 1 - 2 * core, me), device_id_type=MESH)

    def outgoing():
        found = []
        for q in range(pieces_half):
            for k in range(1, n):
                sign = direction(k, q)
                if k <= 2 and (k < n - 1 or n == 2):
                    source = 0
                elif k < n - 1:
                    source = k - 2
                else:
                    source = n - 3 if sign == 1 else n - 2
                found.append((k, q, source, sign))
        return found

    sends = outgoing()

    def start_own():
        for k, q, source, sign in sends:
            if source == 0:
                ring_copy(k, q, pos, sign).start()

    def event(k, q):
        ring_copy(k, q, slot_of(k), direction(k, q)).wait_recv()
        for k2, q2, source, sign in sends:
            if source == k and q2 == q:
                ring_copy(k2, q, slot_of(k), sign).start()
        pair_copy(k, q, core).start()

    per_dir = max(1, (n // 2) * pieces_half - pieces_half // 2)
    events = {}
    for k in range(1, n):
        for q in range(pieces_half):
            if k == n - 1 and direction(k, q) == -1:
                m = (n // 2 - 1) * pieces_half + q - split
            else:
                m = ((k + 1) // 2 - 1) * pieces_half + q
            at = math.ceil(0.18 * steps + 0.65 * steps * (m + 1) / per_dir)
            at = max(1, min(at, steps - 1, lag + k * per_block))
            events.setdefault(at, []).append((m, k, q))

    def v_product(v):
        block = v // per_block
        count = tile // piece_rows
        rhs = gath[slot_of(block), pl.ds((v % per_block) * count, count)].reshape(tile, 2 * bands)
        return jnp.dot(ubuf[v], rhs, preferred_element_type=jnp.float32)

    def await_pair(k):
        for q in range(pieces_half):
            pair_copy(k, q, 1 - core).wait_recv()

    def step(t, with_v):
        slot = lax.rem(t, BUFFERS)
        ahead = t + BUFFERS - 1

        @pl.when(ahead < steps)
        def _():
            for c in w_copies(ahead, lax.rem(ahead, BUFFERS)):
                c.start()

        for at, group in sorted(events.items()):
            if (at >= lag) == with_v:
                @pl.when(t == at)
                def _(group=group):
                    for _m, k, q in sorted(group):
                        event(k, q)
        if with_v:
            for k in range(1, n):
                if lag + k * per_block < steps:
                    @pl.when(t == lag + k * per_block)
                    def _(k=k):
                        await_pair(k)
        for c in w_copies(t, slot):
            c.wait()
        if with_v:
            acc[...] += v_product(t - lag)
        lhs = left[...]
        ur = ui = None
        for j in range(fi + fr):
            tr = jnp.dot(lhs, wbuf[slot, 0, j], preferred_element_type=jnp.float32)
            ti = jnp.dot(lhs, wbuf[slot, 1, j], preferred_element_type=jnp.float32)
            w = weights[j]
            a = w * (tr[:bands] + ti[bands:])
            b = w * (ti[:bands] - tr[bands:])
            ur = a if ur is None else ur + a
            ui = b if ui is None else ui + b
        for i, value in enumerate((ur, ui)):
            high = value.astype(jnp.bfloat16)
            low = (value - high.astype(jnp.float32)).astype(jnp.bfloat16)
            ubuf[t, pl.ds(2 * i * bands, bands), :] = high
            ubuf[t, pl.ds((2 * i + 1) * bands, bands), :] = low

    step(0, False)
    pl.semaphore_wait(barrier, devices - 1)
    start_own()

    def early(t, carry):
        step(t, False)
        return carry

    def late(t, carry):
        step(t, True)
        return carry

    lax.fori_loop(1, lag, early, 0)
    lax.fori_loop(lag, steps, late, 0)

    for k in range(1, n):
        if lag + k * per_block >= steps:
            await_pair(k)
    total = acc[...]
    for v in range(steps - lag, steps):
        total = total + v_product(v)
    p = total[:bands] + total[bands:2 * bands]
    q = total[2 * bands:3 * bands] + total[3 * bands:]
    real = p[:, :bands] - q[:, bands:]
    imag = p[:, bands:] + q[:, :bands]
    share = out_ref.shape[0]
    for d in range(devices):
        stage[d, :, pl.ds(0, bands)] = real[d * share:(d + 1) * share]
        stage[d, :, pl.ds(bands, bands)] = imag[d * share:(d + 1) * share]

    def give(r, carry):
        other = lax.rem(mine + r, devices)
        pltpu.make_async_remote_copy(
            src_ref=stage.at[other], dst_ref=inbox.at[r - 1], send_sem=out_send, recv_sem=out_recv,
            device_id=(other // n, other % n), device_id_type=MESH).start()
        return carry

    lax.fori_loop(1, devices, give, 0)
    for k, q_, source, sign in sends:
        ring_copy(k, q_, pos if source == 0 else slot_of(source), sign).wait_send()
    for k in range(1, n):
        for q_ in range(pieces_half):
            pair_copy(k, q_, core).wait_send()
    pltpu.make_async_copy(inbox, inbox, out_recv).wait()
    out_ref[...] = stage[mine] + jnp.sum(inbox[...], axis=0)
    pltpu.make_async_copy(inbox, inbox, out_send).wait()


def on_device(n, nf, w_imag, w_real, pair_elements, quad_weight, residue_freq, owner_bands):
    fi, rows, width = w_imag.shape
    fr = w_real.shape[0]
    bands = owner_bands.shape[0]
    tile = min(512, rows)
    pieces_half = 2 if rows >= 1024 else 1
    piece_rows = rows // (2 * pieces_half)
    steps = n * (rows // tile)
    devices = n * nf
    share = bands // devices
    dma = pltpu.SemaphoreType.DMA
    anyspace = pl.BlockSpec(memory_space=pl.ANY)
    vmem = pl.BlockSpec(memory_space=pltpu.VMEM)
    flops = 2 * (fi + fr) * rows * width * 2 * bands
    return pl.pallas_call(
        functools.partial(self_energy_kernel, n, nf, pieces_half, tile),
        out_shape=jax.ShapeDtypeStruct((share, 2 * bands), jnp.float32),
        in_specs=[anyspace, anyspace, anyspace, vmem, vmem, vmem],
        out_specs=vmem,
        scratch_shapes=[
            pltpu.VMEM((BUFFERS, 2, fi + fr, rows, tile), jnp.bfloat16),
            pltpu.VMEM((n, 2 * pieces_half, piece_rows, 2 * bands), jnp.bfloat16),
            pltpu.VMEM((2 * bands, rows), jnp.bfloat16),
            pltpu.VMEM((fi + fr, bands, 1), jnp.float32),
            pltpu.VMEM((steps, 4 * bands, tile), jnp.bfloat16),
            pltpu.VMEM((4 * bands, 2 * bands), jnp.float32),
            pltpu.VMEM((devices, share, 2 * bands), jnp.float32),
            pltpu.VMEM((devices - 1, share, 2 * bands), jnp.float32),
            dma((BUFFERS, 2, 2)),
            dma((2 * pieces_half,)),
            dma((n, pieces_half)),
            dma((n, pieces_half)),
            dma((n, pieces_half)),
            dma((n, pieces_half)),
            dma,
            dma,
        ],
        compiler_params=pltpu.CompilerParams(
            collective_id=0, has_side_effects=True, vmem_limit_bytes=60 * 1024 * 1024),
        cost_estimate=pl.CostEstimate(
            flops=flops, bytes_accessed=(fi + fr) * rows * width * 2, transcendentals=0),
    )(w_imag, w_real, pair_elements, quad_weight,
      residue_freq.reshape(1, bands), owner_bands.reshape(1, bands))


def solution(mesh):
    placed = (
        P("freq", "gblk", None),
        P("freq", "gblk", None),
        P("gblk", None),
        P("freq", None),
        P(),
        P(),
    )
    body = functools.partial(on_device, mesh.shape["gblk"], mesh.shape["freq"])
    return jax.shard_map(
        body, mesh=mesh, in_specs=placed, out_specs=P(("freq", "gblk"), None), check_vma=False
    )
```
